32 devices in a mesh: dp: 16 (over z, y, x), feat: 2 (over core).
Axes of the slice: x: 2, y: 2, z: 4, core: 2. Of those that a mesh axis runs over, the one named last changes fastest.
Arguments:
- samples: bfloat16 [4096, 16384], P('dp', 'feat'), may hold values from -1 to 1
- labels: int32 [4096], P('dp'), may hold values from -1 to 1, as said below
- dual: float32 [4096], P('dp'), may hold values from 0 to 1
- counts: int32 [16], P('dp'), may hold values from 1 to 2, as said below
- order: int32 [16, 2], P('dp'), may hold values from 0 to 1, each once within a row
- weights: float32 [16384], P('feat'), may hold values from -0.046875 to 0.046875
Outputs:
- weights_new: float32 [16384], P('feat')
- dual_new: float32 [4096], P('dp')
- margins: float32 [4096], P('dp')
- gap: float32 [], replicated
The draws below stay inside these ranges and needn't reach their ends.
Inputs may be any that keep to these rules, and one draw needn't show every extreme that they name: `labels`: each entry is -1 or 1. `counts`: some index of dp has exactly 2 live blocks.
All inputs are finite; a program needn't handle non-finite values.
Results may differ from the reference program's by a relative error of at most 0.003.
Values sent between devices are 32-bit elements; how exact they have to be, the bound alone decides.
A program may use at most 64 MiB of HBM per device.

```python
import math
import jax
import jax.numpy as jnp
from jax import lax

D = 16384
BLOCK = 128
CAP = 2
PASSES = 2
ROWS = 4096
N_DP = 16


def draw_labels(key, part):
    return (2 * jax.random.randint(key, (ROWS,), 0, 2) - 1).astype(jnp.int32)


def draw_counts(key, part):
    first, second = jax.random.split(jax.random.fold_in(key, 17))
    base = jax.random.randint(first, (N_DP,), 1, CAP + 1)
    where = jax.random.randint(second, (), 0, N_DP)
    return base.at[where].set(CAP).astype(jnp.int32)


def draw_samples(key, part):
    block_total = ROWS // BLOCK
    row_index = jnp.arange(BLOCK, dtype=jnp.int32)
    offset = (row_index[:, None] - row_index[None, :]).astype(jnp.float32)
    first_column = (row_index[None, :] == 0).astype(jnp.float32)
    base_key = jax.random.fold_in(key, 29)

    def one_block(index):
        block_key = jax.random.fold_in(base_key, index)
        rate_key, noise_key = jax.random.split(block_key, 2)
        persist = jax.random.uniform(rate_key, (), jnp.float32, 0.7, 0.9)
        noise = jnp.clip(jax.random.normal(noise_key, (BLOCK, D), jnp.float32), -6.0, 6.0)
        powers = jnp.where(offset >= 0.0, persist ** jnp.maximum(offset, 0.0), 0.0)
        column_scale = first_column + (1.0 - first_column) * jnp.sqrt(1.0 - persist * persist)
        mixing = powers * column_scale
        chained = jnp.dot(mixing, noise, precision=lax.Precision.HIGHEST)
        scaled_rows = jnp.clip(chained / math.sqrt(D), -1.0, 1.0)
        return scaled_rows.astype(jnp.bfloat16)
    blocks = lax.map(one_block, jnp.arange(block_total, dtype=jnp.int32))
    return blocks.reshape(ROWS, D)


def levels(stream_key, shape, cuts, least, high):
    gain = 1.0
    for dim, shards_of in cuts:
        steps = jax.random.uniform(jax.random.fold_in(jax.random.fold_in(stream_key, 6), dim), (shards_of,), jnp.float32, least / len(cuts), high / len(cuts))
        gain = gain * jnp.repeat(jnp.exp(steps), shape[dim] // shards_of).reshape((-1,) + (1,) * (len(shape) - 1 - dim))
    return gain


def scatter_about(rng, shape, spread, reach, cuts=(), kind=jnp.bfloat16):
    loudness = levels(rng, shape, cuts, -0.22, 0.18) if cuts else 1.0
    values = jax.random.normal(rng, shape, jnp.float32) * spread * loudness
    return jnp.minimum(jnp.maximum(values, -reach), reach).astype(kind)


def setup_inputs(seed: int = 0) -> dict:
    arg_keys = jax.random.split(jax.random.key(seed), 7)
    return {
        "samples": draw_samples(jax.random.fold_in(arg_keys[6], 71), 0),
        "labels": draw_labels(jax.random.fold_in(arg_keys[6], 71), 0),
        "dual": jnp.clip(1.0 * jax.random.uniform(arg_keys[2], (ROWS,), jnp.float32) ** levels(arg_keys[2], (ROWS,), ((0, 16),), -0.2, 0.2), 0.0, 1.0),
        "counts": draw_counts(jax.random.fold_in(arg_keys[6], 71), 0),
        "order": jax.vmap(lambda own: jax.random.permutation(own, CAP))(jax.random.split(arg_keys[4], N_DP)).reshape((N_DP, CAP)).astype(jnp.int32),
        "weights": scatter_about(arg_keys[5], (D,), D ** -0.5, 0.046875, ((0, 2),), jnp.float32),
    }


def block_solve(system, right):
    factor = jnp.linalg.cholesky(system)
    lower_part = lax.linalg.triangular_solve(factor, right[:, None], left_side=True, lower=True)
    result = lax.linalg.triangular_solve(factor, lower_part, left_side=True, lower=True, transpose_a=True)
    return result[:, 0]

def local_round(blocks_x, ylab, beta, count, visit, weights, scale):
    grams = jnp.einsum('brd,bsd->brs', blocks_x.astype(jnp.float32), blocks_x.astype(jnp.float32))

    def advance(carry, step):
        beta, change = carry
        slot = visit[step % CAP].astype(jnp.int32)
        rows = lax.dynamic_index_in_dim(blocks_x, slot, 0, keepdims=False)
        gram = lax.dynamic_index_in_dim(grams, slot, 0, keepdims=False)
        start = (slot * BLOCK).astype(jnp.int32)
        signs = lax.dynamic_slice_in_dim(ylab, start, BLOCK).astype(jnp.float32)
        before = lax.dynamic_slice_in_dim(beta, start, BLOCK)
        vector = (weights + change).astype(jnp.bfloat16)
        margin = jnp.dot(rows.astype(jnp.float32), vector.astype(jnp.float32), preferred_element_type=jnp.float32)
        system = jnp.eye(BLOCK, dtype=jnp.float32) + scale * (signs[:, None] * signs[None, :]) * gram
        delta = block_solve(system, 1.0 - before - signs * margin)
        after = jnp.where(slot < count, jnp.maximum(before + delta, 0.0), before)
        scaled = (signs * (after - before)).astype(jnp.bfloat16)
        change = change + scale * jnp.dot(scaled.astype(jnp.float32), rows.astype(jnp.float32), preferred_element_type=jnp.float32)
        beta = lax.dynamic_update_slice_in_dim(beta, after, start, 0)
        return ((beta, change), None)
    init = (beta, jnp.zeros((blocks_x.shape[2],), jnp.float32))
    (beta, change), _ = lax.scan(advance, init, jnp.arange(PASSES * CAP, dtype=jnp.int32))
    return (beta, change)

def reference(samples, labels, dual, counts, order, weights):
    reg = 1.0 / 384.0
    total = jnp.sum(counts.astype(jnp.float32)) * BLOCK
    scale = N_DP / (reg * total)
    grouped = samples.reshape(N_DP, CAP, BLOCK, D)
    ylab = labels.reshape(N_DP, CAP * BLOCK)
    beta0 = dual.reshape(N_DP, CAP * BLOCK)

    def one_group(args):
        blocks_x, signs, beta, count, visit = args
        return local_round(blocks_x, signs, beta, count, visit, weights, scale)
    betas, changes = lax.map(one_group, (grouped, ylab, beta0, counts, order))
    weights_new = weights + jnp.sum(changes, axis=0) / N_DP
    dual_new = betas.reshape(ROWS)
    margins = jnp.dot(samples.astype(jnp.float32), weights_new.astype(jnp.bfloat16).astype(jnp.float32), preferred_element_type=jnp.float32)
    slots = jnp.arange(ROWS, dtype=jnp.int32)
    live = slots // BLOCK % CAP < jnp.repeat(counts, CAP * BLOCK)
    signs = labels.astype(jnp.float32)
    hinge = jnp.maximum(1.0 - signs * margins, 0.0)
    loss = jnp.sum(jnp.where(live, 0.5 * hinge * hinge, 0.0))
    dualsum = jnp.sum(jnp.where(live, dual_new - 0.5 * dual_new * dual_new, 0.0))
    norm = jnp.sum(weights_new * weights_new)
    gap = reg * norm + (loss - dualsum) / total
    return (weights_new, dual_new, margins, gap)
```

```python
import functools

import jax
import jax.numpy as jnp
from jax import lax
from jax.experimental import pallas as pl
from jax.experimental.pallas import tpu as pltpu
from jax.sharding import PartitionSpec as P

BLOCK = 128
CAP = 2
PASSES = 2
LANES = 128
LOAD = 1024
REG = 1.0 / 384.0
MESH = pl.DeviceIdType.MESH
F32 = jnp.float32
BF16 = jnp.bfloat16


def dot_t(a, b):
    return lax.dot_general(a, b, (((1,), (1,)), ((), ())), preferred_element_type=F32)


def dot_full(a, b):
    return lax.dot_general(
        a,
        b,
        (((1,), (0,)), ((), ())),
        preferred_element_type=F32,
        precision=lax.Precision.HIGHEST,
    )


def iterations(features):
    low = 1.0 / (1.0 + features / REG)
    count = 0
    while low < 1.0 - 1e-6:
        low = 4.0 * low / (1.0 + low) ** 2
        count += 1
    return count


def to_row(col, eye):
    return jnp.sum(jnp.where(eye, col, 0.0), axis=0, keepdims=True)


def to_col(row, eye):
    return jnp.sum(jnp.where(eye, row, 0.0), axis=1, keepdims=True)


def two_rows(first, second):
    width = first.shape[1]
    index = lax.broadcasted_iota(jnp.int32, (16, width), 0)
    wide = jnp.where(index == 0, first, jnp.where(index == 1, second, 0.0))
    return wide.astype(BF16)


def split(row):
    high = row.astype(BF16).astype(F32)
    return two_rows(high, row - high)


def kernel(
    groups,
    owners,
    rounds,
    counts_ref,
    order_ref,
    x_hbm,
    w_ref,
    y_ref,
    dual_ref,
    wn_ref,
    dn_ref,
    mg_ref,
    gap_ref,
    xs,
    gram_mine,
    gram_other,
    cnt_mine,
    cnt_all,
    u_mine,
    u_all,
    wn_mine,
    wn_all,
    f_mine,
    f_other,
    t_mine,
    t_all,
    load_sem,
    send_sem,
    recv_sem,
    fsend_sem,
    frecv_sem,
):
    me = lax.axis_index("dp")
    half_id = lax.axis_index("feat")
    partner = 1 - half_id
    rows, half = xs.shape
    chunk = half // owners
    loads = half // LOAD

    def load(i):
        cols = pl.ds(i * LOAD, LOAD)
        return pltpu.make_async_copy(x_hbm.at[:, cols], xs.at[:, cols], load_sem.at[i])

    for i in range(loads):
        load(i).start()

    barrier = pltpu.get_barrier_semaphore()

    def greet(k, _):
        pl.semaphore_signal(
            barrier, inc=1, device_id={"dp": lax.rem(me + k, groups)}, device_id_type=MESH
        )
        return 0

    lax.fori_loop(1, groups, greet, 0)
    pl.semaphore_signal(barrier, inc=1, device_id={"feat": partner}, device_id_type=MESH)

    def send_to(phase, peer, src, dst):
        return pltpu.make_async_remote_copy(
            src_ref=src,
            dst_ref=dst,
            send_sem=send_sem.at[phase, peer],
            recv_sem=recv_sem.at[phase, me],
            device_id={"dp": peer},
            device_id_type=MESH,
        )

    def recv_from(phase, peer, dst):
        return pltpu.make_async_remote_copy(
            src_ref=dst,
            dst_ref=dst,
            send_sem=send_sem.at[phase, peer],
            recv_sem=recv_sem.at[phase, peer],
            device_id={"dp": peer},
            device_id_type=MESH,
        )

    def others(fn):
        def one(k, _):
            fn(lax.rem(me + k, groups))
            return 0

        lax.fori_loop(1, groups, one, 0)

    def if_owner(index, fn):
        if owners == groups:
            fn()
        else:
            pl.when(index < owners)(fn)

    count = counts_ref[0]
    cnt_mine[...] = jnp.full((1, LANES), count.astype(F32), F32)
    eye = lax.broadcasted_iota(jnp.int32, (BLOCK, BLOCK), 0) == lax.broadcasted_iota(
        jnp.int32, (BLOCK, BLOCK), 1
    )

    total = None
    for i in range(loads):
        cols = pl.ds(i * LOAD, LOAD)
        load(i).wait()
        part = xs[:, cols]
        left = jnp.concatenate([part, split(w_ref[:, cols])], axis=0)
        product = dot_t(left, part)
        total = product if total is None else total + product
    gram_mine[...] = total

    pl.semaphore_wait(barrier, groups)

    feat_copy = pltpu.make_async_remote_copy(
        src_ref=gram_mine,
        dst_ref=gram_other,
        send_sem=fsend_sem.at[0],
        recv_sem=frecv_sem.at[0],
        device_id={"feat": partner},
        device_id_type=MESH,
    )
    others(lambda p: send_to(0, p, cnt_mine, cnt_all.at[me]).start())
    feat_copy.start()

    slots = [order_ref[0, v] for v in range(CAP)]

    def pick(items, slot):
        value = items[0]
        for s in range(1, CAP):
            value = jnp.where(slot == s, items[s], value)
        return value

    y_rows = [y_ref[s : s + 1, :].astype(F32) for s in range(CAP)]
    b_rows = [dual_ref[s : s + 1, :] for s in range(CAP)]
    y_row = [pick(y_rows, slot) for slot in slots]
    b_row = [pick(b_rows, slot) for slot in slots]
    y_col = [to_col(r, eye) for r in y_row]
    b_col = [to_col(r, eye) for r in b_row]

    others(lambda p: recv_from(0, p, cnt_all.at[p]).wait_recv())
    cnt_all[me] = cnt_mine[...]
    live_blocks = lax.fori_loop(
        0, groups, lambda i, acc: acc + cnt_all[i], jnp.zeros((1, LANES), F32)
    )
    samples_total = live_blocks * BLOCK
    scale = groups / (REG * samples_total)

    feat_copy.wait()
    full = gram_mine[...] + gram_other[...]
    first = full[rows : rows + 1, :] + full[rows + 1 : rows + 2, :]
    m_rows = [first[:, s * BLOCK : (s + 1) * BLOCK] for s in range(CAP)]
    m_row = [pick(m_rows, slot) for slot in slots]

    def block(r, s):
        return full[r * BLOCK : (r + 1) * BLOCK, s * BLOCK : (s + 1) * BLOCK]

    grams = [
        [
            pick([pick([block(r, s) for s in range(CAP)], slots[b]) for r in range(CAP)], slots[a])
            for b in range(CAP)
        ]
        for a in range(CAP)
    ]

    systems, carry = [], []
    for v in range(CAP):
        system = jnp.where(eye, 1.0, 0.0) + scale * grams[v][v]
        top = jnp.max(jnp.sum(jnp.abs(system), axis=0, keepdims=True), axis=1, keepdims=True)
        low = 1.0 / top
        step = 2.0 / (1.0 + low) * low
        carry.append(step * (jnp.where(eye, 2.0, 0.0) - step * system))
        carry.append(4.0 * low / ((1.0 + low) * (1.0 + low)))
        systems.append(system)

    def improve(_, state):
        new = []
        for v in range(CAP):
            inverse, low = state[2 * v], state[2 * v + 1]
            mu = 2.0 / (1.0 + low)
            near = dot_full(systems[v], inverse)
            new.append(mu * (2.0 * inverse - mu * dot_full(inverse, near)))
            new.append(low * mu * mu)
        return tuple(new)

    carry = lax.fori_loop(1, rounds, improve, tuple(carry))
    inverses = [carry[2 * v] for v in range(CAP)]

    moved = [None] * CAP
    for j in range(PASSES * CAP):
        a = j % CAP
        margin = m_row[a]
        for b in range(CAP):
            if moved[b] is not None:
                margin = margin + scale * jnp.sum(grams[b][a] * moved[b], axis=0, keepdims=True)
        right = y_row[a] * (1.0 - b_row[a] - y_row[a] * margin)
        delta = y_col[a] * jnp.sum(inverses[a] * right, axis=1, keepdims=True)
        after = jnp.where(slots[a] < count, jnp.maximum(b_col[a] + delta, 0.0), b_col[a])
        scaled = (y_col[a] * (after - b_col[a])).astype(BF16).astype(F32)
        moved[a] = scaled if moved[a] is None else moved[a] + scaled
        b_col[a] = after
        b_row[a] = to_row(after, eye)

    def by_slot(items, s):
        value = items[0]
        for v in range(1, CAP):
            value = jnp.where(slots[v] == s, items[v], value)
        return value

    moved_row = [to_row(m, eye) for m in moved]
    beta_rows = [by_slot(b_row, s) for s in range(CAP)]
    for s in range(CAP):
        dn_ref[s : s + 1, :] = beta_rows[s]
    steps = split(jnp.concatenate([by_slot(moved_row, s) for s in range(CAP)], axis=1))

    scale_one = scale[:, 0:1]
    for i in range(owners):
        out = lax.dot_general(
            steps,
            xs[:, i * chunk : (i + 1) * chunk],
            (((1,), (0,)), ((), ())),
            preferred_element_type=F32,
        )
        u_mine[i] = scale_one * (out[0:1, :] + out[1:2, :])

        @pl.when(me != i)
        def _(i=i):
            send_to(1, i, u_mine.at[i], u_all.at[me]).start()

    def reduce_own():
        others(lambda p: recv_from(1, p, u_all.at[p]).wait_recv())
        u_all[me] = u_mine[me]
        summed = lax.fori_loop(
            0, groups, lambda i, acc: acc + u_all[i], jnp.zeros((1, chunk), F32)
        )
        mine = w_ref[:, pl.ds(pl.multiple_of(me * chunk, LANES), chunk)] + summed / groups
        wn_mine[...] = mine
        others(lambda p: send_to(2, p, wn_mine, wn_all.at[me]).start())
        wn_all[me] = mine
        norm = jnp.sum(mine * mine, axis=1, keepdims=True)
        f_mine[:, rows:] = jnp.broadcast_to(norm, (1, LANES))

    if owners != groups:
        f_mine[:, rows:] = jnp.zeros((1, LANES), F32)
    if_owner(me, reduce_own)

    scores = jnp.zeros((16, rows), F32)
    for i in range(owners):

        @pl.when(me != i)
        def _(i=i):
            recv_from(2, i, wn_all.at[i]).wait_recv()

        value = wn_all[i]
        wn_ref[i] = value
        index = lax.broadcasted_iota(jnp.int32, (16, chunk), 0)
        left = jnp.where(index == 0, value, 0.0).astype(BF16)
        scores = scores + dot_t(left, xs[:, i * chunk : (i + 1) * chunk])
    f_mine[:, :rows] = scores[0:1, :]

    margin_copy = pltpu.make_async_remote_copy(
        src_ref=f_mine,
        dst_ref=f_other,
        send_sem=fsend_sem.at[1],
        recv_sem=frecv_sem.at[1],
        device_id={"feat": partner},
        device_id_type=MESH,
    )
    margin_copy.start()
    dual_part = jnp.zeros((1, BLOCK), F32)
    for s in range(CAP):
        beta = beta_rows[s]
        dual_part = dual_part + jnp.where(s < count, beta - 0.5 * beta * beta, 0.0)
    margin_copy.wait()
    both = f_mine[...] + f_other[...]
    loss_part = jnp.zeros((1, BLOCK), F32)
    for s in range(CAP):
        margins = both[:, s * BLOCK : (s + 1) * BLOCK]
        mg_ref[s : s + 1, :] = margins
        hinge = jnp.maximum(1.0 - y_rows[s] * margins, 0.0)
        loss_part = loss_part + jnp.where(s < count, 0.5 * hinge * hinge, 0.0)
    spread = jnp.sum(loss_part - dual_part, axis=1, keepdims=True)
    t_mine[...] = REG * both[:, rows:] + spread / samples_total
    others(lambda p: send_to(3, p, t_mine, t_all.at[me]).start())
    t_all[me] = t_mine[...]
    others(lambda p: recv_from(3, p, t_all.at[p]).wait_recv())
    gap = lax.fori_loop(0, groups, lambda i, acc: acc + t_all[i], jnp.zeros((1, LANES), F32))
    gap_ref[...] = gap

    def drain(p):
        send_to(0, p, cnt_mine, cnt_all.at[me]).wait_send()
        if_owner(p, lambda: send_to(1, p, u_mine.at[p], u_all.at[me]).wait_send())
        if_owner(me, lambda: send_to(2, p, wn_mine, wn_all.at[me]).wait_send())
        send_to(3, p, t_mine, t_all.at[me]).wait_send()

    others(drain)


def body(groups, features, samples, labels, dual, counts, order, weights):
    rows, half = samples.shape
    owners = min(groups, half // LANES)
    chunk = half // owners
    vmem = pl.BlockSpec(memory_space=pltpu.VMEM)
    smem = pl.BlockSpec(memory_space=pltpu.SMEM)
    tall = rows + 16
    wn, dn, mg, gap = pl.pallas_call(
        functools.partial(kernel, groups, owners, iterations(features)),
        out_shape=(
            jax.ShapeDtypeStruct((owners, 1, chunk), F32),
            jax.ShapeDtypeStruct((CAP, BLOCK), F32),
            jax.ShapeDtypeStruct((CAP, BLOCK), F32),
            jax.ShapeDtypeStruct((1, LANES), F32),
        ),
        in_specs=[smem, smem, pl.BlockSpec(memory_space=pl.ANY), vmem, vmem, vmem],
        out_specs=(vmem, vmem, vmem, vmem),
        scratch_shapes=[
            pltpu.VMEM((rows, half), BF16),
            pltpu.VMEM((tall, rows), F32),
            pltpu.VMEM((tall, rows), F32),
            pltpu.VMEM((1, LANES), F32),
            pltpu.VMEM((groups, 1, LANES), F32),
            pltpu.VMEM((owners, 1, chunk), F32),
            pltpu.VMEM((groups, 1, chunk), F32),
            pltpu.VMEM((1, chunk), F32),
            pltpu.VMEM((owners, 1, chunk), F32),
            pltpu.VMEM((1, rows + LANES), F32),
            pltpu.VMEM((1, rows + LANES), F32),
            pltpu.VMEM((1, LANES), F32),
            pltpu.VMEM((groups, 1, LANES), F32),
            pltpu.SemaphoreType.DMA((half // LOAD,)),
            pltpu.SemaphoreType.DMA((4, groups)),
            pltpu.SemaphoreType.DMA((4, groups)),
            pltpu.SemaphoreType.DMA((2,)),
            pltpu.SemaphoreType.DMA((2,)),
        ],
        compiler_params=pltpu.CompilerParams(collective_id=0, has_side_effects=True),
    )(
        counts,
        order,
        samples,
        weights.reshape(1, half),
        labels.reshape(CAP, BLOCK),
        dual.reshape(CAP, BLOCK),
    )
    return (wn.reshape(half), dn.reshape(rows), mg.reshape(rows), gap[0, 0])


def solution(mesh):
    groups = mesh.shape["dp"]
    halves = mesh.shape["feat"]

    def run(samples, *rest):
        return body(groups, samples.shape[1] * halves, samples, *rest)

    return jax.shard_map(
        run,
        mesh=mesh,
        in_specs=(P("dp", "feat"), P("dp"), P("dp"), P("dp"), P("dp", None), P("feat")),
        out_specs=(P("feat"), P("dp"), P("dp"), P()),
        check_vma=False,
    )
```

```python
import functools

import jax
import jax.numpy as jnp
from jax import lax
from jax.experimental import pallas as pl
from jax.experimental.pallas import tpu as pltpu
from jax.sharding import PartitionSpec as P

BLOCK = 128
CAP = 2
PASSES = 2
LANES = 128
LOAD = 1024
REG = 1.0 / 384.0
MESH = pl.DeviceIdType.MESH
F32 = jnp.float32
BF16 = jnp.bfloat16


def dot_t(a, b):
    return lax.dot_general(a, b, (((1,), (1,)), ((), ())), preferred_element_type=F32)


def dot_plain(a, b):
    return lax.dot_general(a, b, (((1,), (0,)), ((), ())), preferred_element_type=F32)


def parts(x):
    one = x.astype(BF16)
    rest = x - one.astype(F32)
    two = rest.astype(BF16)
    return one, two, (rest - two.astype(F32)).astype(BF16)


def as_left(p):
    return jnp.concatenate([p[0], p[1]], axis=1), jnp.concatenate([p[0], p[2]], axis=1)


def as_right(p):
    pair = jnp.concatenate([p[0], p[1]], axis=1)
    return jnp.concatenate([pair, pair], axis=0), jnp.concatenate([p[2], p[0]], axis=0)


def dot_full(left, right):
    wide = dot_plain(left[0], right[0])
    return wide[:, :BLOCK] + (wide[:, BLOCK:] + dot_plain(left[1], right[1]))


def iterations(low, goal):
    count = 0
    while low < goal:
        low = 4.0 * low / (1.0 + low) ** 2
        count += 1
    return count


def to_row(col, eye):
    return jnp.sum(jnp.where(eye, col, 0.0), axis=0, keepdims=True)


def to_col(row, eye):
    return jnp.sum(jnp.where(eye, row, 0.0), axis=1, keepdims=True)


def two_rows(first, second):
    width = first.shape[1]
    index = lax.broadcasted_iota(jnp.int32, (16, width), 0)
    wide = jnp.where(index == 0, first, jnp.where(index == 1, second, 0.0))
    return wide.astype(BF16)


def split(row):
    high = row.astype(BF16).astype(F32)
    return two_rows(high, row - high)


def kernel(
    groups,
    owners,
    features,
    counts_ref,
    order_ref,
    x_hbm,
    w_ref,
    y_ref,
    dual_ref,
    wn_ref,
    dn_ref,
    mg_ref,
    gap_ref,
    xs,
    gram_mine,
    gram_other,
    cnt_mine,
    cnt_all,
    u_mine,
    u_all,
    wn_mine,
    wn_all,
    f_mine,
    f_other,
    t_mine,
    t_all,
    load_sem,
    send_sem,
    recv_sem,
    fsend_sem,
    frecv_sem,
):
    me = lax.axis_index("dp")
    half_id = lax.axis_index("feat")
    partner = 1 - half_id
    rows, half = xs.shape
    chunk = half // owners
    loads = half // LOAD

    def load(i):
        cols = pl.ds(i * LOAD, LOAD)
        return pltpu.make_async_copy(x_hbm.at[:, cols], xs.at[:, cols], load_sem.at[i])

    for i in range(loads):
        load(i).start()

    barrier = pltpu.get_barrier_semaphore()

    def greet(k, _):
        pl.semaphore_signal(
            barrier, inc=1, device_id={"dp": lax.rem(me + k, groups)}, device_id_type=MESH
        )
        return 0

    lax.fori_loop(1, groups, greet, 0)
    pl.semaphore_signal(barrier, inc=1, device_id={"feat": partner}, device_id_type=MESH)

    def send_to(phase, peer, src, dst):
        return pltpu.make_async_remote_copy(
            src_ref=src,
            dst_ref=dst,
            send_sem=send_sem.at[phase, peer],
            recv_sem=recv_sem.at[phase, me],
            device_id={"dp": peer},
            device_id_type=MESH,
        )

    def recv_from(phase, peer, dst):
        return pltpu.make_async_remote_copy(
            src_ref=dst,
            dst_ref=dst,
            send_sem=send_sem.at[phase, peer],
            recv_sem=recv_sem.at[phase, peer],
            device_id={"dp": peer},
            device_id_type=MESH,
        )

    def others(fn):
        def one(k, _):
            fn(lax.rem(me + k, groups))
            return 0

        lax.fori_loop(1, groups, one, 0)

    def if_owner(index, fn):
        if owners == groups:
            fn()
        else:
            pl.when(index < owners)(fn)

    count = counts_ref[0]
    cnt_mine[...] = jnp.full((1, LANES), count.astype(F32), F32)
    eye = lax.broadcasted_iota(jnp.int32, (BLOCK, BLOCK), 0) == lax.broadcasted_iota(
        jnp.int32, (BLOCK, BLOCK), 1
    )

    total = None
    for i in range(loads):
        cols = pl.ds(i * LOAD, LOAD)
        load(i).wait()
        part = xs[:, cols]
        left = jnp.concatenate([part, split(w_ref[:, cols])], axis=0)
        product = dot_t(left, part)
        total = product if total is None else total + product
    gram_mine[...] = total

    pl.semaphore_wait(barrier, groups)

    feat_copy = pltpu.make_async_remote_copy(
        src_ref=gram_mine,
        dst_ref=gram_other,
        send_sem=fsend_sem.at[0],
        recv_sem=frecv_sem.at[0],
        device_id={"feat": partner},
        device_id_type=MESH,
    )
    others(lambda p: send_to(0, p, cnt_mine, cnt_all.at[me]).start())
    feat_copy.start()

    slots = [order_ref[0, v] for v in range(CAP)]

    def pick(items, slot):
        value = items[0]
        for s in range(1, CAP):
            value = jnp.where(slot == s, items[s], value)
        return value

    y_rows = [y_ref[s : s + 1, :].astype(F32) for s in range(CAP)]
    b_rows = [dual_ref[s : s + 1, :] for s in range(CAP)]
    y_row = [pick(y_rows, slot) for slot in slots]
    b_row = [pick(b_rows, slot) for slot in slots]
    y_col = [to_col(r, eye) for r in y_row]
    b_col = [to_col(r, eye) for r in b_row]

    feat_copy.wait()
    full = gram_mine[...] + gram_other[...]
    first = full[rows : rows + 1, :] + full[rows + 1 : rows + 2, :]
    m_rows = [first[:, s * BLOCK : (s + 1) * BLOCK] for s in range(CAP)]
    m_row = [pick(m_rows, slot) for slot in slots]

    def block(r, s):
        return full[r * BLOCK : (r + 1) * BLOCK, s * BLOCK : (s + 1) * BLOCK]

    grams = [
        [
            pick([pick([block(r, s) for s in range(CAP)], slots[b]) for r in range(CAP)], slots[a])
            for b in range(CAP)
        ]
        for a in range(CAP)
    ]

    diag = jnp.where(eye, 1.0, 0.0)
    ratio = (CAP * groups / (groups + 1)) ** 0.5
    middle = groups / (REG * BLOCK * CAP * groups) * ratio
    rounds = iterations(1.0 / (1.0 + middle * features * BLOCK), 0.99)
    refines = iterations(0.99 / ratio, 1.0 - 1e-6)

    def improve(lefts, state):
        new = []
        for v in range(CAP):
            inverse, low = state[2 * v], state[2 * v + 1]
            mu = 2.0 / (1.0 + low)
            terms = parts(inverse)
            near = dot_full(lefts[v], as_right(terms))
            far = dot_full(as_left(terms), as_right(parts(near)))
            new.append(mu * (2.0 * inverse - mu * far))
            new.append(low * mu * mu)
        return tuple(new)

    lefts, carry = [], []
    for v in range(CAP):
        system = diag + middle * grams[v][v]
        top = jnp.max(jnp.sum(jnp.abs(system), axis=0, keepdims=True), axis=1, keepdims=True)
        low = 1.0 / top
        step = 2.0 / (1.0 + low) * low
        carry.append(step * (2.0 * diag - step * system))
        carry.append(4.0 * low / ((1.0 + low) * (1.0 + low)))
        lefts.append(as_left(parts(system)))
    carry = lax.fori_loop(1, rounds, lambda _, state: improve(lefts, state), tuple(carry))

    others(lambda p: recv_from(0, p, cnt_all.at[p]).wait_recv())
    cnt_all[me] = cnt_mine[...]
    live_blocks = lax.fori_loop(
        0, groups, lambda i, acc: acc + cnt_all[i], jnp.zeros((1, LANES), F32)
    )
    samples_total = live_blocks * BLOCK
    scale = groups / (REG * samples_total)


    quotient = scale[:, 0:1] / middle
    start = 0.99 * jnp.minimum(quotient, 1.0 / quotient)
    state = []
    for v in range(CAP):
        state.append(carry[2 * v] / jnp.maximum(quotient, 1.0))
        state.append(start)
    lefts = [as_left(parts(diag + scale * grams[v][v])) for v in range(CAP)]
    for _ in range(refines):
        state = improve(lefts, state)
    inverses = [state[2 * v] for v in range(CAP)]

    moved = [None] * CAP
    for j in range(PASSES * CAP):
        a = j % CAP
        margin = m_row[a]
        for b in range(CAP):
            if moved[b] is not None:
                margin = margin + scale * jnp.sum(grams[b][a] * moved[b], axis=0, keepdims=True)
        right = y_row[a] * (1.0 - b_row[a] - y_row[a] * margin)
        delta = y_col[a] * jnp.sum(inverses[a] * right, axis=1, keepdims=True)
        after = jnp.where(slots[a] < count, jnp.maximum(b_col[a] + delta, 0.0), b_col[a])
        scaled = (y_col[a] * (after - b_col[a])).astype(BF16).astype(F32)
        moved[a] = scaled if moved[a] is None else moved[a] + scaled
        b_col[a] = after
        b_row[a] = to_row(after, eye)

    def by_slot(items, s):
        value = items[0]
        for v in range(1, CAP):
            value = jnp.where(slots[v] == s, items[v], value)
        return value

    moved_row = [to_row(m, eye) for m in moved]
    beta_rows = [by_slot(b_row, s) for s in range(CAP)]
    for s in range(CAP):
        dn_ref[s : s + 1, :] = beta_rows[s]
    steps = split(jnp.concatenate([by_slot(moved_row, s) for s in range(CAP)], axis=1))

    scale_one = scale[:, 0:1]
    for i in range(owners):
        out = lax.dot_general(
            steps,
            xs[:, i * chunk : (i + 1) * chunk],
            (((1,), (0,)), ((), ())),
            preferred_element_type=F32,
        )
        u_mine[i] = scale_one * (out[0:1, :] + out[1:2, :])

        @pl.when(me != i)
        def _(i=i):
            send_to(1, i, u_mine.at[i], u_all.at[me]).start()

    def reduce_own():
        others(lambda p: recv_from(1, p, u_all.at[p]).wait_recv())
        u_all[me] = u_mine[me]
        summed = lax.fori_loop(
            0, groups, lambda i, acc: acc + u_all[i], jnp.zeros((1, chunk), F32)
        )
        mine = w_ref[:, pl.ds(pl.multiple_of(me * chunk, LANES), chunk)] + summed / groups
        wn_mine[...] = mine
        others(lambda p: send_to(2, p, wn_mine, wn_all.at[me]).start())
        wn_all[me] = mine
        norm = jnp.sum(mine * mine, axis=1, keepdims=True)
        f_mine[:, rows:] = jnp.broadcast_to(norm, (1, LANES))

    if owners != groups:
        f_mine[:, rows:] = jnp.zeros((1, LANES), F32)
    if_owner(me, reduce_own)

    scores = jnp.zeros((16, rows), F32)
    for i in range(owners):

        @pl.when(me != i)
        def _(i=i):
            recv_from(2, i, wn_all.at[i]).wait_recv()

        value = wn_all[i]
        wn_ref[i] = value
        index = lax.broadcasted_iota(jnp.int32, (16, chunk), 0)
        left = jnp.where(index == 0, value, 0.0).astype(BF16)
        scores = scores + dot_t(left, xs[:, i * chunk : (i + 1) * chunk])
    f_mine[:, :rows] = scores[0:1, :]

    margin_copy = pltpu.make_async_remote_copy(
        src_ref=f_mine,
        dst_ref=f_other,
        send_sem=fsend_sem.at[1],
        recv_sem=frecv_sem.at[1],
        device_id={"feat": partner},
        device_id_type=MESH,
    )
    margin_copy.start()
    dual_part = jnp.zeros((1, BLOCK), F32)
    for s in range(CAP):
        beta = beta_rows[s]
        dual_part = dual_part + jnp.where(s < count, beta - 0.5 * beta * beta, 0.0)
    margin_copy.wait()
    both = f_mine[...] + f_other[...]
    loss_part = jnp.zeros((1, BLOCK), F32)
    for s in range(CAP):
        margins = both[:, s * BLOCK : (s + 1) * BLOCK]
        mg_ref[s : s + 1, :] = margins
        hinge = jnp.maximum(1.0 - y_rows[s] * margins, 0.0)
        loss_part = loss_part + jnp.where(s < count, 0.5 * hinge * hinge, 0.0)
    spread = jnp.sum(loss_part - dual_part, axis=1, keepdims=True)
    t_mine[...] = REG * both[:, rows:] + spread / samples_total
    others(lambda p: send_to(3, p, t_mine, t_all.at[me]).start())
    t_all[me] = t_mine[...]
    others(lambda p: recv_from(3, p, t_all.at[p]).wait_recv())
    gap = lax.fori_loop(0, groups, lambda i, acc: acc + t_all[i], jnp.zeros((1, LANES), F32))
    gap_ref[...] = gap

    def drain(p):
        send_to(0, p, cnt_mine, cnt_all.at[me]).wait_send()
        if_owner(p, lambda: send_to(1, p, u_mine.at[p], u_all.at[me]).wait_send())
        if_owner(me, lambda: send_to(2, p, wn_mine, wn_all.at[me]).wait_send())
        send_to(3, p, t_mine, t_all.at[me]).wait_send()

    others(drain)


def hand_over(*refs):
    count = len(refs) // 2
    for source, target in zip(refs[:count], refs[count:]):
        target[...] = source[...]


def body(groups, features, samples, labels, dual, counts, order, weights):
    rows, half = samples.shape
    owners = min(groups, half // LANES)
    chunk = half // owners
    vmem = pl.BlockSpec(memory_space=pltpu.VMEM)
    smem = pl.BlockSpec(memory_space=pltpu.SMEM)
    tall = rows + 16
    wn, dn, mg, gap = pl.pallas_call(
        functools.partial(kernel, groups, owners, features),
        out_shape=(
            jax.ShapeDtypeStruct((owners, 1, chunk), F32),
            jax.ShapeDtypeStruct((CAP, BLOCK), F32),
            jax.ShapeDtypeStruct((CAP, BLOCK), F32),
            jax.ShapeDtypeStruct((1, LANES), F32),
        ),
        in_specs=[smem, smem, pl.BlockSpec(memory_space=pl.ANY), vmem, vmem, vmem],
        out_specs=(vmem, vmem, vmem, vmem),
        scratch_shapes=[
            pltpu.VMEM((rows, half), BF16),
            pltpu.VMEM((tall, rows), F32),
            pltpu.VMEM((tall, rows), F32),
            pltpu.VMEM((1, LANES), F32),
            pltpu.VMEM((groups, 1, LANES), F32),
            pltpu.VMEM((owners, 1, chunk), F32),
            pltpu.VMEM((groups, 1, chunk), F32),
            pltpu.VMEM((1, chunk), F32),
            pltpu.VMEM((owners, 1, chunk), F32),
            pltpu.VMEM((1, rows + LANES), F32),
            pltpu.VMEM((1, rows + LANES), F32),
            pltpu.VMEM((1, LANES), F32),
            pltpu.VMEM((groups, 1, LANES), F32),
            pltpu.SemaphoreType.DMA((half // LOAD,)),
            pltpu.SemaphoreType.DMA((4, groups)),
            pltpu.SemaphoreType.DMA((4, groups)),
            pltpu.SemaphoreType.DMA((2,)),
            pltpu.SemaphoreType.DMA((2,)),
        ],
        compiler_params=pltpu.CompilerParams(collective_id=0, has_side_effects=True),
    )(
        counts,
        order,
        samples,
        weights.reshape(1, half),
        labels.reshape(CAP, BLOCK),
        dual.reshape(CAP, BLOCK),
    )
    results = (wn, dn, mg, gap)
    wn, dn, mg, gap = pl.pallas_call(
        hand_over,
        out_shape=tuple(jax.ShapeDtypeStruct(r.shape, r.dtype) for r in results),
        in_specs=[vmem] * len(results),
        out_specs=(vmem,) * len(results),
    )(*results)
    return (wn.reshape(half), dn.reshape(rows), mg.reshape(rows), gap[0, 0])


def solution(mesh):
    groups = mesh.shape["dp"]
    halves = mesh.shape["feat"]

    def run(samples, *rest):
        return body(groups, samples.shape[1] * halves, samples, *rest)

    return jax.shard_map(
        run,
        mesh=mesh,
        in_specs=(P("dp", "feat"), P("dp"), P("dp"), P("dp"), P("dp", None), P("feat")),
        out_specs=(P("feat"), P("dp"), P("dp"), P()),
        check_vma=False,
    )
```

```python
import functools

import jax
import jax.numpy as jnp
from jax import lax
from jax.experimental import pallas as pl
from jax.experimental.pallas import tpu as pltpu
from jax.sharding import PartitionSpec as P

BLOCK = 128
CAP = 2
PASSES = 2
LANES = 128
LOAD = 1024
REG = 1.0 / 384.0
MESH = pl.DeviceIdType.MESH
F32 = jnp.float32
BF16 = jnp.bfloat16


def dot_t(a, b):
    return lax.dot_general(a, b, (((1,), (1,)), ((), ())), preferred_element_type=F32)


def dot_plain(a, b):
    return lax.dot_general(a, b, (((1,), (0,)), ((), ())), preferred_element_type=F32)


def parts(x):
    one = x.astype(BF16)
    rest = x - one.astype(F32)
    two = rest.astype(BF16)
    return one, two, (rest - two.astype(F32)).astype(BF16)


def as_left(p):
    return jnp.concatenate([p[0], p[1]], axis=1), jnp.concatenate([p[0], p[2]], axis=1)


def as_right(p):
    pair = jnp.concatenate([p[0], p[1]], axis=1)
    return jnp.concatenate([pair, pair], axis=0), jnp.concatenate([p[2], p[0]], axis=0)


def dot_full(left, right, short):
    wide = dot_plain(left[0], right[0])
    if short:
        return wide[:, :BLOCK] + wide[:, BLOCK:]
    return wide[:, :BLOCK] + (wide[:, BLOCK:] + dot_plain(left[1], right[1]))


def iterations(low, goal):
    count = 0
    while low < goal:
        low = 4.0 * low / (1.0 + low) ** 2
        count += 1
    return count


def to_row(col, eye):
    return jnp.sum(jnp.where(eye, col, 0.0), axis=0, keepdims=True)


def to_col(row, eye):
    return jnp.sum(jnp.where(eye, row, 0.0), axis=1, keepdims=True)


def two_rows(first, second):
    width = first.shape[1]
    index = lax.broadcasted_iota(jnp.int32, (16, width), 0)
    wide = jnp.where(index == 0, first, jnp.where(index == 1, second, 0.0))
    return wide.astype(BF16)


def split(row):
    high = row.astype(BF16).astype(F32)
    return two_rows(high, row - high)


def kernel(
    groups,
    owners,
    features,
    counts_ref,
    order_ref,
    x_hbm,
    w_ref,
    y_ref,
    dual_ref,
    wn_ref,
    dn_ref,
    mg_ref,
    gap_ref,
    xs,
    gram_mine,
    gram_other,
    cnt_mine,
    cnt_all,
    u_mine,
    u_all,
    wn_mine,
    wn_all,
    f_mine,
    f_other,
    t_mine,
    t_all,
    load_sem,
    send_sem,
    recv_sem,
    fsend_sem,
    frecv_sem,
):
    me = lax.axis_index("dp")
    half_id = lax.axis_index("feat")
    partner = 1 - half_id
    rows, half = xs.shape
    chunk = half // owners
    loads = half // LOAD

    def load(i):
        cols = pl.ds(i * LOAD, LOAD)
        return pltpu.make_async_copy(x_hbm.at[:, cols], xs.at[:, cols], load_sem.at[i])

    for i in range(loads):
        load(i).start()

    barrier = pltpu.get_barrier_semaphore()

    def greet(k, _):
        pl.semaphore_signal(
            barrier, inc=1, device_id={"dp": lax.rem(me + k, groups)}, device_id_type=MESH
        )
        return 0

    lax.fori_loop(1, groups, greet, 0)
    pl.semaphore_signal(barrier, inc=1, device_id={"feat": partner}, device_id_type=MESH)

    def send_to(phase, peer, src, dst):
        return pltpu.make_async_remote_copy(
            src_ref=src,
            dst_ref=dst,
            send_sem=send_sem.at[phase, peer],
            recv_sem=recv_sem.at[phase, me],
            device_id={"dp": peer},
            device_id_type=MESH,
        )

    def recv_from(phase, peer, dst):
        return pltpu.make_async_remote_copy(
            src_ref=dst,
            dst_ref=dst,
            send_sem=send_sem.at[phase, peer],
            recv_sem=recv_sem.at[phase, peer],
            device_id={"dp": peer},
            device_id_type=MESH,
        )

    def others(fn):
        def one(k, _):
            fn(lax.rem(me + k, groups))
            return 0

        lax.fori_loop(1, groups, one, 0)

    def if_owner(index, fn):
        if owners == groups:
            fn()
        else:
            pl.when(index < owners)(fn)

    count = counts_ref[0]
    cnt_mine[...] = jnp.full((1, LANES), count.astype(F32), F32)
    eye = lax.broadcasted_iota(jnp.int32, (BLOCK, BLOCK), 0) == lax.broadcasted_iota(
        jnp.int32, (BLOCK, BLOCK), 1
    )

    total = None
    for i in range(loads):
        cols = pl.ds(i * LOAD, LOAD)
        load(i).wait()
        part = xs[:, cols]
        left = jnp.concatenate([part, split(w_ref[:, cols])], axis=0)
        product = dot_t(left, part)
        total = product if total is None else total + product
    gram_mine[...] = total

    pl.semaphore_wait(barrier, groups)

    feat_copy = pltpu.make_async_remote_copy(
        src_ref=gram_mine,
        dst_ref=gram_other,
        send_sem=fsend_sem.at[0],
        recv_sem=frecv_sem.at[0],
        device_id={"feat": partner},
        device_id_type=MESH,
    )
    others(lambda p: send_to(0, p, cnt_mine, cnt_all.at[me]).start())
    feat_copy.start()

    slots = [order_ref[0, v] for v in range(CAP)]

    def pick(items, slot):
        value = items[0]
        for s in range(1, CAP):
            value = jnp.where(slot == s, items[s], value)
        return value

    y_rows = [y_ref[s : s + 1, :].astype(F32) for s in range(CAP)]
    b_rows = [dual_ref[s : s + 1, :] for s in range(CAP)]
    y_row = [pick(y_rows, slot) for slot in slots]
    b_row = [pick(b_rows, slot) for slot in slots]
    y_col = [to_col(r, eye) for r in y_row]
    b_col = [to_col(r, eye) for r in b_row]

    feat_copy.wait()
    full = gram_mine[...] + gram_other[...]
    first = full[rows : rows + 1, :] + full[rows + 1 : rows + 2, :]
    m_rows = [first[:, s * BLOCK : (s + 1) * BLOCK] for s in range(CAP)]
    m_row = [pick(m_rows, slot) for slot in slots]

    def block(r, s):
        return full[r * BLOCK : (r + 1) * BLOCK, s * BLOCK : (s + 1) * BLOCK]

    grams = [
        [
            pick([pick([block(r, s) for s in range(CAP)], slots[b]) for r in range(CAP)], slots[a])
            for b in range(CAP)
        ]
        for a in range(CAP)
    ]

    diag = jnp.where(eye, 1.0, 0.0)
    ratio = (CAP * groups / (groups + 1)) ** 0.5
    middle = groups / (REG * BLOCK * CAP * groups) * ratio
    rounds = iterations(1.0 / (1.0 + middle * features * BLOCK), 0.99)
    refines = iterations(0.99 / ratio, 1.0 - 1e-6)

    def improve(lefts, state, short=False):
        new = []
        for v in range(CAP):
            inverse, low = state[2 * v], state[2 * v + 1]
            mu = 2.0 / (1.0 + low)
            terms = parts(inverse)
            near = dot_full(lefts[v], as_right(terms), short)
            far = dot_full(as_left(terms), as_right(parts(near)), short)
            new.append(mu * (2.0 * inverse - mu * far))
            new.append(low * mu * mu)
        return tuple(new)

    lefts, carry = [], []
    for v in range(CAP):
        system = diag + middle * grams[v][v]
        top = jnp.max(jnp.sum(jnp.abs(system), axis=0, keepdims=True), axis=1, keepdims=True)
        low = 1.0 / top
        step = 2.0 / (1.0 + low) * low
        carry.append(step * (2.0 * diag - step * system))
        carry.append(4.0 * low / ((1.0 + low) * (1.0 + low)))
        lefts.append(as_left(parts(system)))
    for k in range(1, rounds):
        carry = improve(lefts, carry, short=k <= 5)

    others(lambda p: recv_from(0, p, cnt_all.at[p]).wait_recv())
    cnt_all[me] = cnt_mine[...]
    live_blocks = lax.fori_loop(
        0, groups, lambda i, acc: acc + cnt_all[i], jnp.zeros((1, LANES), F32)
    )
    samples_total = live_blocks * BLOCK
    scale = groups / (REG * samples_total)


    quotient = scale[:, 0:1] / middle
    start = 0.99 * jnp.minimum(quotient, 1.0 / quotient)
    state = []
    for v in range(CAP):
        state.append(carry[2 * v] / jnp.maximum(quotient, 1.0))
        state.append(start)
    lefts = [as_left(parts(diag + scale * grams[v][v])) for v in range(CAP)]
    for _ in range(refines):
        state = improve(lefts, state)
    inverses = [state[2 * v] for v in range(CAP)]

    moved = [None] * CAP
    for j in range(PASSES * CAP):
        a = j % CAP
        margin = m_row[a]
        for b in range(CAP):
            if moved[b] is not None:
                margin = margin + scale * jnp.sum(grams[b][a] * moved[b], axis=0, keepdims=True)
        right = y_row[a] * (1.0 - b_row[a] - y_row[a] * margin)
        delta = y_col[a] * jnp.sum(inverses[a] * right, axis=1, keepdims=True)
        after = jnp.where(slots[a] < count, jnp.maximum(b_col[a] + delta, 0.0), b_col[a])
        scaled = (y_col[a] * (after - b_col[a])).astype(BF16).astype(F32)
        moved[a] = scaled if moved[a] is None else moved[a] + scaled
        b_col[a] = after
        b_row[a] = to_row(after, eye)

    def by_slot(items, s):
        value = items[0]
        for v in range(1, CAP):
            value = jnp.where(slots[v] == s, items[v], value)
        return value

    moved_row = [to_row(m, eye) for m in moved]
    beta_rows = [by_slot(b_row, s) for s in range(CAP)]
    for s in range(CAP):
        dn_ref[s : s + 1, :] = beta_rows[s]
    steps = split(jnp.concatenate([by_slot(moved_row, s) for s in range(CAP)], axis=1))

    scale_one = scale[:, 0:1]
    for i in range(owners):
        out = lax.dot_general(
            steps,
            xs[:, i * chunk : (i + 1) * chunk],
            (((1,), (0,)), ((), ())),
            preferred_element_type=F32,
        )
        u_mine[i] = scale_one * (out[0:1, :] + out[1:2, :])

        @pl.when(me != i)
        def _(i=i):
            send_to(1, i, u_mine.at[i], u_all.at[me]).start()

    def reduce_own():
        others(lambda p: recv_from(1, p, u_all.at[p]).wait_recv())
        u_all[me] = u_mine[me]
        summed = lax.fori_loop(
            0, groups, lambda i, acc: acc + u_all[i], jnp.zeros((1, chunk), F32)
        )
        mine = w_ref[:, pl.ds(pl.multiple_of(me * chunk, LANES), chunk)] + summed / groups
        wn_mine[...] = mine
        others(lambda p: send_to(2, p, wn_mine, wn_all.at[me]).start())
        wn_all[me] = mine
        norm = jnp.sum(mine * mine, axis=1, keepdims=True)
        f_mine[:, rows:] = jnp.broadcast_to(norm, (1, LANES))

    if owners != groups:
        f_mine[:, rows:] = jnp.zeros((1, LANES), F32)
    if_owner(me, reduce_own)

    scores = jnp.zeros((16, rows), F32)
    for i in range(owners):

        @pl.when(me != i)
        def _(i=i):
            recv_from(2, i, wn_all.at[i]).wait_recv()

        value = wn_all[i]
        wn_ref[i] = value
        index = lax.broadcasted_iota(jnp.int32, (16, chunk), 0)
        left = jnp.where(index == 0, value, 0.0).astype(BF16)
        scores = scores + dot_t(left, xs[:, i * chunk : (i + 1) * chunk])
    f_mine[:, :rows] = scores[0:1, :]

    margin_copy = pltpu.make_async_remote_copy(
        src_ref=f_mine,
        dst_ref=f_other,
        send_sem=fsend_sem.at[1],
        recv_sem=frecv_sem.at[1],
        device_id={"feat": partner},
        device_id_type=MESH,
    )
    margin_copy.start()
    dual_part = jnp.zeros((1, BLOCK), F32)
    for s in range(CAP):
        beta = beta_rows[s]
        dual_part = dual_part + jnp.where(s < count, beta - 0.5 * beta * beta, 0.0)
    margin_copy.wait()
    both = f_mine[...] + f_other[...]
    loss_part = jnp.zeros((1, BLOCK), F32)
    for s in range(CAP):
        margins = both[:, s * BLOCK : (s + 1) * BLOCK]
        mg_ref[s : s + 1, :] = margins
        hinge = jnp.maximum(1.0 - y_rows[s] * margins, 0.0)
        loss_part = loss_part + jnp.where(s < count, 0.5 * hinge * hinge, 0.0)
    spread = jnp.sum(loss_part - dual_part, axis=1, keepdims=True)
    t_mine[...] = REG * both[:, rows:] + spread / samples_total
    others(lambda p: send_to(3, p, t_mine, t_all.at[me]).start())
    t_all[me] = t_mine[...]
    others(lambda p: recv_from(3, p, t_all.at[p]).wait_recv())
    gap = lax.fori_loop(0, groups, lambda i, acc: acc + t_all[i], jnp.zeros((1, LANES), F32))
    gap_ref[...] = gap

    def drain(p):
        send_to(0, p, cnt_mine, cnt_all.at[me]).wait_send()
        if_owner(p, lambda: send_to(1, p, u_mine.at[p], u_all.at[me]).wait_send())
        if_owner(me, lambda: send_to(2, p, wn_mine, wn_all.at[me]).wait_send())
        send_to(3, p, t_mine, t_all.at[me]).wait_send()

    others(drain)


def hand_over(*refs):
    count = len(refs) // 2
    for source, target in zip(refs[:count], refs[count:]):
        target[...] = source[...]


def body(groups, features, samples, labels, dual, counts, order, weights):
    rows, half = samples.shape
    owners = min(groups, half // LANES)
    chunk = half // owners
    vmem = pl.BlockSpec(memory_space=pltpu.VMEM)
    smem = pl.BlockSpec(memory_space=pltpu.SMEM)
    tall = rows + 16
    wn, dn, mg, gap = pl.pallas_call(
        functools.partial(kernel, groups, owners, features),
        out_shape=(
            jax.ShapeDtypeStruct((owners, 1, chunk), F32),
            jax.ShapeDtypeStruct((CAP, BLOCK), F32),
            jax.ShapeDtypeStruct((CAP, BLOCK), F32),
            jax.ShapeDtypeStruct((1, LANES), F32),
        ),
        in_specs=[smem, smem, pl.BlockSpec(memory_space=pl.ANY), vmem, vmem, vmem],
        out_specs=(vmem, vmem, vmem, vmem),
        scratch_shapes=[
            pltpu.VMEM((rows, half), BF16),
            pltpu.VMEM((tall, rows), F32),
            pltpu.VMEM((tall, rows), F32),
            pltpu.VMEM((1, LANES), F32),
            pltpu.VMEM((groups, 1, LANES), F32),
            pltpu.VMEM((owners, 1, chunk), F32),
            pltpu.VMEM((groups, 1, chunk), F32),
            pltpu.VMEM((1, chunk), F32),
            pltpu.VMEM((owners, 1, chunk), F32),
            pltpu.VMEM((1, rows + LANES), F32),
            pltpu.VMEM((1, rows + LANES), F32),
            pltpu.VMEM((1, LANES), F32),
            pltpu.VMEM((groups, 1, LANES), F32),
            pltpu.SemaphoreType.DMA((half // LOAD,)),
            pltpu.SemaphoreType.DMA((4, groups)),
            pltpu.SemaphoreType.DMA((4, groups)),
            pltpu.SemaphoreType.DMA((2,)),
            pltpu.SemaphoreType.DMA((2,)),
        ],
        compiler_params=pltpu.CompilerParams(collective_id=0, has_side_effects=True),
    )(
        counts,
        order,
        samples,
        weights.reshape(1, half),
        labels.reshape(CAP, BLOCK),
        dual.reshape(CAP, BLOCK),
    )
    results = (wn, dn, mg, gap)
    wn, dn, mg, gap = pl.pallas_call(
        hand_over,
        out_shape=tuple(jax.ShapeDtypeStruct(r.shape, r.dtype) for r in results),
        in_specs=[vmem] * len(results),
        out_specs=(vmem,) * len(results),
    )(*results)
    return (wn.reshape(half), dn.reshape(rows), mg.reshape(rows), gap[0, 0])


def solution(mesh):
    groups = mesh.shape["dp"]
    halves = mesh.shape["feat"]

    def run(samples, *rest):
        return body(groups, samples.shape[1] * halves, samples, *rest)

    return jax.shard_map(
        run,
        mesh=mesh,
        in_specs=(P("dp", "feat"), P("dp"), P("dp"), P("dp"), P("dp", None), P("feat")),
        out_specs=(P("feat"), P("dp"), P("dp"), P()),
        check_vma=False,
    )
```
